256 devices in a mesh: row: 32 (over y_lo, z, core), col: 8 (over y_hi, x).
Axes of the slice: x: 4, y: 4 (y_hi: 2, y_lo: 2; y = y_hi * 2 + y_lo), z: 8, core: 2. Of those that a mesh axis runs over, the one named last changes fastest.
Arguments:
- embeddings: bfloat16 [491520, 768], P(('row', 'col')), may hold values from -1 to 1, as said below
- valid: int32 [491520], P(('row', 'col')), may hold values 0 or 1
Outputs:
- best_match: float32 [491520], P(('row', 'col'))
- near_count: float32 [491520], P(('row', 'col'))
The draws below stay inside these ranges and needn't reach their ends.
Inputs may be any that keep to these rules, and one draw needn't show every extreme that they name: `embeddings`: each row has length 1 up to bfloat16 rounding.
All inputs are finite; a program needn't handle non-finite values. No bound on the sum of `valid` on one device may be relied on, other than what follows from the above.
Results may differ from the reference program's by a relative error of at most 0.01.
Values may be sent and summed in bfloat16 or wider, within the bound.
A program may use at most 64 MiB of HBM per device.

```python
import jax
import jax.numpy as jnp
from jax import lax

D = 768
BLOCK = 1920
STEPS = 3
GRID_ROWS = 32
GRID_COLS = 8
MEMBERS = 491520


def draw_embeddings(key, part):
    keys = jax.random.split(key, 7)
    base = jax.random.normal(keys[0], (MEMBERS, D), jnp.float32)
    low_level, high_level = (0.15, 1.5)
    base = base / jnp.sqrt(jnp.sum(base * base, axis=1, keepdims=True) + 1e-06)
    blocks = MEMBERS // BLOCK
    member = jnp.arange(MEMBERS, dtype=jnp.int32)
    owner = member // BLOCK
    grid_a = owner // GRID_COLS
    grid_c = owner % GRID_COLS
    inner = member % BLOCK
    offset = jax.random.randint(keys[1], (blocks,), 0, STEPS, dtype=jnp.int32)[owner]
    rowshift = jax.random.randint(keys[2], (blocks,), 1, max(BLOCK, 2), dtype=jnp.int32)[owner]
    partner = ((grid_a - offset) % GRID_ROWS * GRID_COLS + (grid_c + offset) % GRID_COLS) * BLOCK + (inner + rowshift) % BLOCK
    chosen = jax.random.randint(keys[3], (MEMBERS,), 0, 4, dtype=jnp.int32) == 0
    level = jnp.exp(jax.random.uniform(keys[4], (MEMBERS,), jnp.float32, jnp.log(low_level), jnp.log(high_level)))
    noise = jax.random.normal(keys[5], (MEMBERS, D), jnp.float32)
    noise = noise / jnp.sqrt(jnp.sum(noise * noise, axis=1, keepdims=True) + 1e-06)
    copied = base[partner] + level[:, None] * noise
    copied = copied / jnp.sqrt(jnp.sum(copied * copied, axis=1, keepdims=True) + 1e-06)
    return jnp.where(chosen[:, None], copied, base).astype(jnp.bfloat16)


def touch_ends(drawn, rng, smallest, top_value):
    shape = drawn.shape
    spot = [jax.random.randint(jax.random.fold_in(rng, axis), (), 0, shape[axis]) for axis in range(len(shape))]
    drawn = drawn.at[tuple(spot)].set(smallest)
    longest = shape.index(max(shape))
    spot[longest] = (spot[longest] + 1) % shape[longest]
    return drawn.at[tuple(spot)].set(top_value)


def setup_inputs(seed: int = 0) -> dict:
    streams_of = jax.random.split(jax.random.key(seed), 3)
    return {
        "embeddings": draw_embeddings(jax.random.fold_in(streams_of[2], 71), 0),
        "valid": touch_ends((jax.random.randint(streams_of[1], (MEMBERS,), 0, 8) < 7).astype(jnp.int32), jax.random.fold_in(streams_of[1], 1), 0, 1),
    }


THRESHOLD = 0.6
SHARPNESS = 0.05


def reference(embeddings, valid):
    grid_emb = embeddings.reshape(GRID_ROWS, GRID_COLS, BLOCK, D)
    grid_valid = valid.reshape(GRID_ROWS, GRID_COLS, BLOCK)
    rows = jnp.arange(BLOCK, dtype=jnp.int32)

    def one_block(index):
        grid_a = index // GRID_COLS
        grid_c = index % GRID_COLS
        query = grid_emb[grid_a, grid_c]
        best = jnp.full((BLOCK,), -1.0, jnp.float32)
        count = jnp.zeros((BLOCK,), jnp.float32)
        for step in range(STEPS):
            cand_a = ((grid_a - step) % GRID_ROWS).astype(jnp.int32)
            cand_c = ((grid_c + step) % GRID_COLS).astype(jnp.int32)
            cand = grid_emb[cand_a, cand_c]
            scores = lax.dot_general(query, cand, (((1,), (1,)), ((), ())), preferred_element_type=jnp.float32)
            allowed = grid_valid[cand_a, cand_c][None, :] > 0
            if step == 0:
                allowed = allowed & (rows[:, None] != rows[None, :])
            best = jnp.maximum(best, jnp.max(jnp.where(allowed, scores, -1.0), axis=1))
            soft = jax.nn.sigmoid((scores - THRESHOLD) / SHARPNESS)
            count = count + jnp.sum(jnp.where(allowed, soft, 0.0), axis=1)
        return best, count

    best_all, count_all = lax.map(one_block, jnp.arange(GRID_ROWS * GRID_COLS, dtype=jnp.int32))
    return best_all.reshape(MEMBERS), count_all.reshape(MEMBERS)
```

```python
import jax
import jax.numpy as jnp
from jax import lax
from jax.experimental import pallas as pl
from jax.experimental.pallas import tpu as pltpu
from jax.sharding import PartitionSpec as P

MESH = pl.DeviceIdType.MESH
THRESHOLD = 0.6
SHARPNESS = 0.05
LOG2E = 1.4426950408889634

PARTS = 1
RELAYS = 2
PIECE = 48
GROUP = PARTS * PIECE
TILE = 384
AHEAD = 4
LAG_R, LAG_H, LAG_B, LAG_Z, LAG_D = (2, 4), 7, 10, 13, 14

SENDS = [
    0, 25, 1, 27, 16, 10, 18, 11, 8, 1, 26, 2, 59, 17, 11, 19,
    1, 9, 2, 27, 16, 58, 18, 8, 24, 2, 10, 3, 11, 17, 57, 19,
    2, 25, 3, 11, 0, 8, 18, 56, 24, 3, 26, 0, 8, 1, 9, 19,
    3, 25, 0, 27, 16, 9, 2, 10, 24, 0, 26, 1, 9, 17, 10, 3,
    0, 25, 1, 27, 16, 10, 18, 11, 8, 1, 26, 2, 59, 17, 11, 19,
    1, 9, 2, 27, 16, 58, 18, 8, 24, 2, 10, 3, 11, 17, 57, 19,
    2, 25, 3, 11, 0, 8, 18, 56, 24, 3, 26, 0, 8, 1, 9, 19,
    3, 25, 0, 27, 16, 9, 2, 10, 24, 0, 26, 1, 9, 17, 10, 3,
    4, 29, 5, 31, 20, 14, 22, 15, 12, 5, 30, 6, 63, 21, 15, 23,
    5, 13, 6, 31, 20, 62, 22, 12, 28, 6, 14, 7, 15, 21, 61, 23,
    6, 29, 7, 15, 4, 12, 22, 60, 28, 7, 30, 4, 12, 5, 13, 23,
    7, 29, 4, 31, 20, 13, 6, 14, 28, 4, 30, 5, 13, 21, 14, 7,
    4, 29, 5, 31, 20, 14, 22, 15, 12, 5, 30, 6, 63, 21, 15, 23,
    5, 13, 6, 31, 20, 62, 22, 12, 28, 6, 14, 7, 15, 21, 61, 23,
    6, 29, 7, 15, 4, 12, 22, 60, 28, 7, 30, 4, 12, 5, 13, 23,
    7, 29, 4, 31, 20, 13, 6, 14, 28, 4, 30, 5, 13, 21, 14, 7,
]
RELAYED = [
    17, 0, 25, 0, 74752, 65, 0, 449, 0, 25, 0, 1, 0, 0, 73, 82944,
    25, 0, 1, 0, 0, 0, 91136, 81, 0, 1, 0, 9, 73, 66560, 0, 0,
    0, 0, 9, 0, 74752, 81, 0, 0, 0, 0, 0, 17, 473, 0, 89, 82944,
    9, 0, 0, 0, 0, 465, 91136, 65, 0, 17, 0, 0, 89, 66560, 457, 0,
    17, 0, 25, 0, 74752, 65, 0, 449, 0, 25, 0, 1, 0, 0, 73, 82944,
    25, 0, 1, 0, 0, 0, 91136, 81, 0, 1, 0, 9, 73, 66560, 0, 0,
    0, 0, 9, 0, 74752, 81, 0, 0, 0, 0, 0, 17, 473, 0, 89, 82944,
    9, 0, 0, 0, 0, 465, 91136, 65, 0, 17, 0, 0, 89, 66560, 457, 0,
    49, 0, 57, 0, 107520, 97, 0, 481, 0, 57, 0, 33, 0, 0, 105, 115712,
    57, 0, 33, 0, 0, 0, 123904, 113, 0, 33, 0, 41, 105, 99328, 0, 0,
    0, 0, 41, 0, 107520, 113, 0, 0, 0, 0, 0, 49, 505, 0, 121, 115712,
    41, 0, 0, 0, 0, 497, 123904, 97, 0, 49, 0, 0, 121, 99328, 489, 0,
    49, 0, 57, 0, 107520, 97, 0, 481, 0, 57, 0, 33, 0, 0, 105, 115712,
    57, 0, 33, 0, 0, 0, 123904, 113, 0, 33, 0, 41, 105, 99328, 0, 0,
    0, 0, 41, 0, 107520, 113, 0, 0, 0, 0, 0, 49, 505, 0, 121, 115712,
    41, 0, 0, 0, 0, 497, 123904, 97, 0, 49, 0, 0, 121, 99328, 489, 0,
]
HOMES = [
    16, 530, 84, 598, 177, 691, 245, 759, 512, 66, 580, 134, 673, 227, 741, 39,
    64, 578, 132, 646, 225, 739, 37, 551, 576, 130, 644, 198, 737, 35, 549, 103,
    128, 642, 196, 710, 33, 547, 101, 615, 640, 194, 708, 6, 545, 99, 613, 167,
    192, 706, 4, 518, 97, 611, 165, 679, 704, 2, 516, 70, 609, 163, 677, 231,
    0, 514, 68, 582, 161, 675, 229, 743, 512, 66, 580, 134, 673, 227, 741, 39,
    64, 578, 132, 646, 225, 739, 37, 551, 576, 130, 644, 198, 737, 35, 549, 103,
    128, 642, 196, 710, 33, 547, 101, 615, 640, 194, 708, 6, 545, 99, 613, 167,
    192, 706, 4, 518, 97, 611, 165, 679, 720, 18, 532, 86, 625, 179, 693, 247,
    264, 778, 332, 846, 425, 939, 493, 1007, 792, 346, 860, 414, 953, 507, 1021, 319,
    344, 858, 412, 926, 505, 1019, 317, 831, 856, 410, 924, 478, 1017, 315, 829, 383,
    408, 922, 476, 990, 313, 827, 381, 895, 920, 474, 988, 286, 825, 379, 893, 447,
    472, 986, 284, 798, 377, 891, 445, 959, 984, 282, 796, 350, 889, 443, 957, 511,
    280, 794, 348, 862, 441, 955, 509, 1023, 792, 346, 860, 414, 953, 507, 1021, 319,
    344, 858, 412, 926, 505, 1019, 317, 831, 856, 410, 924, 478, 1017, 315, 829, 383,
    408, 922, 476, 990, 313, 827, 381, 895, 920, 474, 988, 286, 825, 379, 893, 447,
    472, 986, 284, 798, 377, 891, 445, 959, 968, 266, 780, 334, 873, 427, 941, 495,
]


def lookup(index):
    words = [jnp.int32(0)] * 3
    for i in range(len(SENDS)):
        hit = index == i
        words = [jnp.where(hit, jnp.int32(t[i]), w) for t, w in zip((SENDS, RELAYED, HOMES), words)]
    return words


def bits(word, low, count):
    return (word // (1 << low)) % (1 << count)


def device(position, z, core):
    x, y = position % 4, position // 4
    return ((y % 2) * 16 + z * 2 + core, (y // 2) * 4 + x)


def kernel(
    emb, valid, best_out, count_out, data, relay, bounce, id_0, id_1, id_own, id_way, weight, acc_best, acc_count, sent, got,
    own_ss, relay_ss, z_ss, b_ss, d_ss, v_ss, s_ss, home_rs, relay_rs, z_rs, b_rs, d_rs, v_rs, s_rs, load_sem, vload_sem,
):
    members = emb.shape[0]
    groups = members // GROUP
    HOME, Z, D, OWN = 0, 1, 2, 3
    row, col = lax.axis_index("row"), lax.axis_index("col")
    core = row % 2
    z = (row // 2) % 8
    here = ((col // 4) * 2 + row // 16) * 4 + col % 4

    load = pltpu.make_async_copy(emb, data.at[OWN], load_sem)
    load.start()
    vload = pltpu.make_async_copy(valid, id_own, vload_sem)
    vload.start()

    barrier = pltpu.get_barrier_semaphore()
    position = ((col // 4) * 2 + row // 16) * 4 + col % 4
    across = position + 4 - 8 * ((position // 4) % 2)
    friends = [(row + 1 - 2 * core, col)]
    friends += [device((position + i) % 16, z, core) for i in range(1, 16)]
    friends += [device(at, (z + i) % 8, core) for i in (1, 2, 6, 7) for at in (position, across)]
    for friend in friends:
        pl.semaphore_signal(barrier, inc=1, device_id=friend, device_id_type=MESH)
    sends, relayed, homes = lookup(row * 8 + col)
    pl.semaphore_wait(barrier, len(friends))

    part_pos = [bits(sends, 7 * p, 4) for p in range(PARTS)]
    part_rel = [bits(sends, 7 * p + 4, 1) == 1 for p in range(PARTS)]
    part_slot = [bits(sends, 7 * p + 5, 2) for p in range(PARTS)]
    part_local = [jnp.logical_and(jnp.logical_not(part_rel[p]), part_pos[p] == here) for p in range(PARTS)]
    part_home = [jnp.logical_and(jnp.logical_not(part_rel[p]), part_pos[p] != here) for p in range(PARTS)]
    slot_on = [bits(relayed, 10 * r, 1) == 1 for r in range(RELAYS)]
    slot_part = [bits(relayed, 10 * r + 1, 2) for r in range(RELAYS)]
    slot_pos = [bits(relayed, 10 * r + 3, 4) for r in range(RELAYS)]
    slot_again = [bits(relayed, 10 * r + 7, 1) == 1 for r in range(RELAYS)]
    chain = bits(homes, 0, 3)
    held_row = bits(homes, 3, 1) * 16 + z * 2 + core
    z_next = (z + 7 + 2 * core) % 8
    z_dev = device(bits(homes, 4, 2) * 4 + col % 4, z_next, core)
    sibling = (row + 1 - 2 * core, col)
    v_pos = bits(homes, 6, 4)
    origin_b = (held_row, (chain - held_row + 64) % 8)
    q_row = (held_row + 2 * (1 - core)) % 32
    origin_a = (q_row, (chain - q_row + 64) % 8)

    def rows(piece):
        return pl.ds(pl.multiple_of(piece * PIECE, PIECE), PIECE)

    def grows(group):
        return pl.ds(pl.multiple_of(group * GROUP, GROUP), GROUP)

    def remote(src, dst, ss, rs, dev):
        return pltpu.make_async_remote_copy(
            src_ref=src, dst_ref=dst, send_sem=ss, recv_sem=rs, device_id=dev, device_id_type=MESH
        )

    def own_send(g):
        for p in range(PARTS):
            piece = g * PARTS + p
            dev = device(part_pos[p], z, core)

            @pl.when(part_local[p])
            def _():
                pltpu.make_async_copy(emb.at[rows(piece)], data.at[HOME, rows(piece)], home_rs.at[piece]).start()

            @pl.when(part_home[p])
            def _():
                remote(emb.at[rows(piece)], data.at[HOME, rows(piece)], own_ss.at[p], home_rs.at[piece], dev).start()

            @pl.when(part_rel[p])
            def _():
                remote(
                    emb.at[rows(piece)], relay.at[part_slot[p], rows(g)], own_ss.at[p],
                    relay_rs.at[part_slot[p], g], dev,
                ).start()

    def relay_send(r, g):
        @pl.when(slot_on[r])
        def _():
            piece = g * PARTS + slot_part[r]
            src = relay.at[r, rows(g)]
            dev = device(slot_pos[r], z, core)
            remote(src, src, relay_ss.at[r], relay_rs.at[r, g], sibling).wait_recv()
            if r + 1 < RELAYS:

                @pl.when(slot_again[r])
                def _():
                    remote(src, relay.at[r + 1, rows(g)], relay_ss.at[r], relay_rs.at[r + 1, g], dev).start()

            @pl.when(jnp.logical_not(slot_again[r]))
            def _():
                remote(src, data.at[HOME, rows(piece)], relay_ss.at[r], home_rs.at[piece], dev).start()

    way = 2 * core - 1
    wraps = z == 7 * core
    bounces = z == 6 - 5 * core
    far_dev = device(bits(homes, 4, 2) * 4 + col % 4, (z_next + way + 8) % 8, core)
    near_dev = device(here, (z - way + 8) % 8, core)

    def z_copy(g):
        return remote(data.at[HOME, grows(g)], data.at[Z, grows(g)], z_ss, z_rs.at[g], z_dev)

    def z_send(g):
        far = jnp.logical_and(wraps, g % 2 == 1)

        @pl.when(far)
        def _():
            remote(data.at[HOME, grows(g)], bounce.at[grows(g // 2)], z_ss, b_rs.at[g // 2], far_dev).start()

        @pl.when(jnp.logical_not(far))
        def _():
            z_copy(g).start()

    def bounce_copy(g):
        return remote(bounce.at[grows(g // 2)], data.at[Z, grows(g)], b_ss, z_rs.at[g], near_dev)

    def bounce_step(g):
        @pl.when(jnp.logical_and(bounces, g % 2 == 1))
        def _():
            src = bounce.at[grows(g // 2)]
            remote(src, src, b_ss, b_rs.at[g // 2], sibling).wait_recv()
            bounce_copy(g).start()

    def d_copy(g, slot):
        return remote(data.at[slot, grows(g)], data.at[D, grows(g)], d_ss, d_rs.at[g], sibling)

    def home_step(g):
        for p in range(PARTS):
            piece = g * PARTS + p
            remote(data.at[HOME, rows(piece)], data.at[HOME, rows(piece)], z_ss, home_rs.at[piece], sibling).wait_recv()
        z_send(g)

        @pl.when(core == 0)
        def _():
            d_copy(g, HOME).start()

    def z_step(g):
        z_copy(g).wait_recv()

        @pl.when(core == 1)
        def _():
            d_copy(g, Z).start()

    for g in range(AHEAD):
        own_send(g)

    v_here = v_pos == here
    for t, target in enumerate((id_0, id_way)):

        @pl.when(jnp.logical_and(core == t, v_here))
        def _():
            pltpu.make_async_copy(valid, target, v_rs.at[2 * t]).start()

        @pl.when(jnp.logical_and(core == t, jnp.logical_not(v_here)))
        def _():
            remote(valid, target, v_ss.at[0], v_rs.at[2 * t], device(v_pos, z, core)).start()

    v_on = remote(id_way, id_0, v_ss.at[1], v_rs.at[0], z_dev)
    v_over = remote(id_0, id_1, v_ss.at[2], v_rs.at[1], sibling)

    def v_step():
        @pl.when(core == 1)
        def _():
            remote(id_way, id_way, v_ss.at[0], v_rs.at[2], sibling).wait_recv()
            v_on.start()

    def v_share():
        v_on.wait_recv()
        v_over.start()

    acc_best[...] = jnp.full(acc_best.shape, -1.0, jnp.float32)
    acc_count[...] = jnp.zeros(acc_count.shape, jnp.float32)

    def spread(slot):
        line = (id_0, id_1, id_own)[slot]
        for i in range(members // 128):
            part = line[i * 128 : (i + 1) * 128].astype(jnp.float32).reshape(1, 128)
            weight[slot, i * 128 : (i + 1) * 128, :] = jnp.broadcast_to(part, (128, 128)).T

    def tiles_of(jobs):
        found = []
        for unit, c_slot, q_slot, c, q, own in jobs:
            c_at = pl.ds(pl.multiple_of(c * TILE, TILE), TILE)
            q_at = pl.ds(pl.multiple_of(q * TILE, TILE), TILE)
            scores = lax.dot_general(
                data[c_slot, c_at, :], data[q_slot, q_at, :], (((1,), (1,)), ((), ())), preferred_element_type=jnp.float32
            )
            w = weight[unit, c_at, :]
            allowed = jnp.concatenate([w] * (TILE // 128), axis=1) > 0.5
            if own:
                shape = (TILE, TILE)
                differ = lax.broadcasted_iota(jnp.int32, shape, 0) != lax.broadcasted_iota(jnp.int32, shape, 1)
                allowed = jnp.logical_and(allowed, differ)
            top = jnp.where(allowed, scores, -1.0).reshape(TILE // 8, 8, TILE)
            soft = 1.0 / (1.0 + jnp.exp2(scores * (-LOG2E / SHARPNESS) + THRESHOLD * LOG2E / SHARPNESS))
            soft = jnp.where(allowed, soft, 0.0).reshape(TILE // 8, 8, TILE)
            found.append((unit, q_at, jnp.max(top, axis=0), jnp.sum(soft, axis=0)))
        for unit, q_at, top, soft in found:
            acc_best[unit, :, q_at] = jnp.maximum(acc_best[unit, :, q_at], top)
            acc_count[unit, :, q_at] = acc_count[unit, :, q_at] + soft

    load.wait()
    vload.wait()
    spread(2)

    tiles = members // TILE
    lag = LAG_D

    def own_tiles(n):
        q = n % tiles

        @pl.when(n < tiles)
        def _():
            tiles_of([(2, OWN, OWN, q, q, True)])

        @pl.when(n >= tiles)
        def _():
            tiles_of([(2, OWN, OWN, (q + n // tiles) % tiles, q, False)])

    def pair_tiles(t, first, last):
        @pl.loop(first, last)
        def _(n):
            late = jnp.where(n <= t + 1, t, n - t - 2)
            held = jnp.where(n <= t + 1, n, t + 1)
            c = jnp.where(core == 0, held, late)
            q = jnp.where(core == 0, late, held)
            tiles_of([(0, core, 1 - core, c, q, False), (1, D, HOME, late, held, False)])

    per = TILE // GROUP

    @pl.loop(0, groups + lag)
    def _(s):
        for r in range(RELAYS):

            @pl.when(jnp.logical_and(s >= LAG_R[r], s < groups + LAG_R[r]))
            def _():
                relay_send(r, s - LAG_R[r])

        @pl.when(jnp.logical_and(s >= LAG_B, s < groups + LAG_B))
        def _():
            bounce_step(s - LAG_B)

        @pl.when(jnp.logical_and(s >= LAG_H, s < groups + LAG_H))
        def _():
            home_step(s - LAG_H)

        @pl.when(s + AHEAD < groups)
        def _():
            own_send(s + AHEAD)

        @pl.when(jnp.logical_and(s >= LAG_Z, s < groups + LAG_Z))
        def _():
            z_step(s - LAG_Z)

        @pl.when(s >= LAG_D)
        def _():
            d_copy(s - LAG_D, HOME).wait_recv()

        @pl.when(s < tiles * tiles)
        def _():
            own_tiles(s)

        @pl.when(s == LAG_H)
        def _():
            v_step()

        @pl.when(s == LAG_Z)
        def _():
            v_share()

        @pl.when(s == LAG_D)
        def _():
            v_over.wait_recv()
            for slot in range(2):
                spread(slot)

        done = s - lag + 1
        t = done // per - 1
        phase = done % per

        @pl.when(t >= 0)
        def _():
            total = jnp.where(t == tiles - 1, tiles, 2 * t + 2)
            pair_tiles(t, total * phase // per, jnp.where(t == tiles - 1, total, total * (phase + 1) // per))

    def folded(unit):
        return (
            jnp.max(acc_best[unit], axis=0, keepdims=True),
            jnp.sum(acc_count[unit], axis=0, keepdims=True),
        )

    for unit in range(2):
        b, n = folded(unit)
        sent[unit, 0:1, :] = b
        sent[unit, 1:2, :] = n
    mine_b, mine_n = folded(2)

    s_dev = [origin_a, origin_b]
    s_copies = [remote(sent.at[u], got.at[u], s_ss.at[u], s_rs.at[u], s_dev[u]) for u in range(2)]
    s_here = [jnp.logical_and(d[0] == row, d[1] == col) for d in s_dev]
    for u in range(2):

        @pl.when(s_here[u])
        def _():
            got[u] = sent[u]

        @pl.when(jnp.logical_not(s_here[u]))
        def _():
            s_copies[u].start()

    z_all = remote(data.at[HOME], data.at[Z], z_ss, z_rs.at[0], z_dev)
    z_all.wait_send()

    @pl.when(bounces)
    def _():
        half = pl.ds(0, groups // 2 * GROUP)
        remote(bounce.at[half], data.at[Z, half], b_ss, z_rs.at[0], near_dev).wait_send()

    remote(data.at[HOME], data.at[D], d_ss, d_rs.at[0], sibling).wait_send()
    part_rows = pl.ds(0, members // PARTS)
    for p in range(PARTS):

        @pl.when(jnp.logical_not(part_local[p]))
        def _():
            remote(emb.at[part_rows], data.at[HOME, part_rows], own_ss.at[p], home_rs.at[0], sibling).wait_send()

    for r in range(RELAYS):

        @pl.when(slot_on[r])
        def _():
            remote(relay.at[r], data.at[HOME, part_rows], relay_ss.at[r], home_rs.at[0], sibling).wait_send()

    @pl.when(jnp.logical_not(v_here))
    def _():
        remote(valid, id_0, v_ss.at[0], v_rs.at[0], sibling).wait_send()

    @pl.when(core == 1)
    def _():
        v_on.wait_send()

    v_over.wait_send()

    for u in range(2):

        @pl.when(jnp.logical_not(s_here[u]))
        def _():
            s_copies[u].wait_send()
            s_copies[u].wait_recv()

    best_out[...] = jnp.maximum(mine_b, jnp.maximum(got[0, 0:1, :], got[1, 0:1, :]))[0]
    count_out[...] = (mine_n + got[0, 1:2, :] + got[1, 1:2, :])[0]


def shards(embeddings, valid):
    members, width = embeddings.shape
    groups = members // GROUP
    dma = pltpu.SemaphoreType.DMA
    best, count = pl.pallas_call(
        kernel,
        out_shape=[jax.ShapeDtypeStruct((members,), jnp.float32)] * 2,
        in_specs=[pl.BlockSpec(memory_space=pl.ANY)] * 2,
        out_specs=[pl.BlockSpec(memory_space=pltpu.VMEM)] * 2,
        scratch_shapes=[
            pltpu.VMEM((4, members, width), jnp.bfloat16),
            pltpu.VMEM((RELAYS, members // PARTS, width), jnp.bfloat16),
            pltpu.VMEM((groups // 2 * GROUP, width), jnp.bfloat16),
            pltpu.VMEM((members,), jnp.int32),
            pltpu.VMEM((members,), jnp.int32),
            pltpu.VMEM((members,), jnp.int32),
            pltpu.VMEM((members,), jnp.int32),
            pltpu.VMEM((3, members, 128), jnp.float32),
            pltpu.VMEM((3, 8, members), jnp.float32),
            pltpu.VMEM((3, 8, members), jnp.float32),
            pltpu.VMEM((3, 2, members), jnp.float32),
            pltpu.VMEM((3, 2, members), jnp.float32),
            dma((PARTS,)),
            dma((RELAYS,)),
            dma,
            dma,
            dma,
            dma((3,)),
            dma((2,)),
            dma((groups * PARTS,)),
            dma((RELAYS, groups)),
            dma((groups,)),
            dma((groups // 2,)),
            dma((groups,)),
            dma((3,)),
            dma((2,)),
            dma,
            dma,
        ],
        compiler_params=pltpu.CompilerParams(collective_id=0, has_side_effects=True, vmem_limit_bytes=60 * 2**20),
    )(embeddings, valid)
    return best, count


def solution(mesh):
    return jax.shard_map(
        shards,
        mesh=mesh,
        in_specs=(P(("row", "col"), None), P(("row", "col"))),
        out_specs=(P(("row", "col")), P(("row", "col"))),
        check_vma=False,
    )
```
